32 devices in a mesh: seq: 8 (over z, x), tp: 4 (over y, core).
Axes of the slice: x: 2, y: 2, z: 4, core: 2. Of those that a mesh axis runs over, the one named last changes fastest.
Arguments:
- tokens: bfloat16 [1024, 4608], P('seq'), may hold values from -6 to 6
- counts: int32 [8], P('seq'), may hold values from 0 to 32, as said below
- selected: int32 [8, 32], P('seq'), may hold values from 0 to 127, as said below
- router_w: float32 [4608], replicated, may hold values from -0.09375 to 0.09375
- pre_gain: float32 [4608], replicated, may hold values from 0.25 to 1.75
- post_gain: float32 [4608], replicated, may hold values from 0.25 to 1.75
- gate_w: bfloat16 [4608, 36864], P(None, ('seq', 'tp')), may hold values from -0.09375 to 0.09375
- up_w: bfloat16 [4608, 36864], P(None, ('seq', 'tp')), may hold values from -0.09375 to 0.09375
- down_w: bfloat16 [36864, 4608], P(('seq', 'tp')), may hold values from -0.0625 to 0.0625
Outputs:
- layer_out: bfloat16 [1024, 4608], P('seq')
The draws below stay inside these ranges and needn't reach their ends.
Inputs may be any that keep to these rules, and one draw needn't show every extreme that they name: The counts sum to 128. For every shard s, the sum of the counts of the shards before s differs from s * 16 by at most 32. Each shard's first counts entries are distinct token positions of that shard in increasing order; the entries after them are padding and name no selected token.
All inputs are finite; a program needn't handle non-finite values.
Results may differ from the reference program's by a relative error of at most 0.003.
Values may be sent and summed in bfloat16 or wider, within the bound.
No kernel may reach another device: no remote copies, remote signals or barrier semaphores. Data moves between devices by JAX's collectives and lax.ppermute only.
A program may use at most 128 MiB of HBM per device.

```python
import jax
import jax.numpy as jnp
from jax import lax

D = 4608
FF = 36864
TOK_DEV = 128
LOAD = 16
CAP = 32
SHARDS = 8
TOKENS = 1024


def draw_counts(key, part):
    shard_count = SHARDS
    slot_count = LOAD
    marked = jax.random.randint(jax.random.fold_in(key, 7), (), 3, shard_count - 2)
    moves = jax.random.randint(jax.random.fold_in(key, 11), (shard_count,), -slot_count, slot_count + 1)
    index = jnp.arange(shard_count)
    lower = jnp.full((shard_count,), -2 * slot_count, jnp.int32)
    upper = jnp.full((shard_count,), 2 * slot_count, jnp.int32)
    lower = jnp.where(index == marked - 3, -slot_count, lower)
    upper = jnp.where(index == marked - 3, slot_count, upper)
    lower = jnp.where(index == marked - 2, 0, lower)
    upper = jnp.where(index == marked - 2, slot_count, upper)
    lower = jnp.where(index == marked - 1, slot_count, lower)
    upper = jnp.where(index == marked - 1, slot_count, upper)
    moves = jnp.where(index == marked, slot_count, moves)
    lower = jnp.where(index == shard_count - 2, -slot_count, lower)
    upper = jnp.where(index == shard_count - 2, slot_count, upper)
    lower = jnp.where(index == shard_count - 1, 0, lower)
    upper = jnp.where(index == shard_count - 1, 0, upper)

    def advance(level, item):
        move_now, low_now, high_now = item
        following = jnp.clip(level + move_now, low_now, high_now)
        return (following, slot_count + following - level)
    final_level, drawn = lax.scan(advance, jnp.int32(0), (moves.astype(jnp.int32), lower, upper))
    return drawn.astype(jnp.int32)


def draw_selected(key, part):
    shard_keys = jax.random.split(jax.random.fold_in(key, 3), SHARDS)

    def one_shard(shard_key):
        order = jax.random.permutation(shard_key, TOK_DEV)
        return jnp.sort(order[:CAP])
    return jax.vmap(one_shard)(shard_keys).astype(jnp.int32)


def raised(values, key, source, target, blocks, factor):
    owner, partner = [(jnp.arange(values.shape[axis_at]) // (values.shape[axis_at] // blocks)).reshape([-1 if axis == axis_at else 1 for axis in range(values.ndim)]) for axis_at in (source, target)]
    chosen = jax.random.permutation(key, blocks)[partner]
    strong = (owner == chosen) | (owner == (partner + blocks // 2) % blocks)
    return jnp.where(strong, factor * values, values)


def steps_of(key, shape, pieces, least, largest):
    def one(dim, blocks):
        steps = jax.random.uniform(jax.random.fold_in(jax.random.fold_in(key, 6), dim), (blocks,), jnp.float32, least / len(pieces), largest / len(pieces))
        return jnp.repeat(jnp.exp(steps), shape[dim] // blocks).reshape((-1,) + (1,) * (len(shape) - dim - 1))

    factor_of = one(*pieces[0])
    for cut in pieces[1:]:
        factor_of = factor_of * one(*cut)
    return factor_of


def gaussian(own_key, extent, width, reach, shards=(), held_as=jnp.bfloat16):
    values = width * jax.random.normal(own_key, extent, jnp.float32)
    if shards:
        values = values * steps_of(own_key, extent, shards, -0.22, 0.18)
    return jnp.clip(values, -reach, reach).astype(held_as)


def noise_with(key, dims, width, limit, cuts, heavy, kind=jnp.bfloat16):
    values = width * jax.random.normal(key, dims, jnp.float32)
    if cuts:
        values = values * steps_of(key, dims, cuts, -0.22, 0.18)
    return jnp.clip(raised(values, jax.random.fold_in(key, 3), *heavy), -limit, limit).astype(kind)


def setup_inputs(seed: int = 0) -> dict:
    streams_of = jax.random.split(jax.random.key(seed), 10)
    tokens = gaussian(streams_of[0], (TOKENS, D), 1.0, 6.0, ((0, 8),))
    counts = draw_counts(jax.random.fold_in(streams_of[9], 71), 0)
    selected = draw_selected(jax.random.fold_in(streams_of[9], 71), 0)
    router_w = gaussian(streams_of[3], (D,), D ** -0.5, 0.09375, (), jnp.float32)
    pre_gain = jnp.clip(1.0 + 0.15 * jax.random.normal(streams_of[4], (D,), jnp.float32), 0.25, 1.75)
    post_gain = jnp.clip(1.0 + 0.15 * jax.random.normal(streams_of[5], (D,), jnp.float32), 0.25, 1.75)
    gate_w = gaussian(streams_of[6], (D, FF), D ** -0.5, 0.09375, ((1, 32),))
    up_w = gaussian(streams_of[7], (D, FF), D ** -0.5, 0.09375, ((1, 32),))
    down_w = noise_with(streams_of[8], (FF, D), FF ** -0.5, 0.0625, ((0, 32),), (0, 1, 32, 2.75))
    return dict(tokens=tokens, counts=counts, selected=selected, router_w=router_w, pre_gain=pre_gain, post_gain=post_gain, gate_w=gate_w, up_w=up_w, down_w=down_w)


EPS = 1e-06

def norm_rows(values, scale_vec):
    return values * lax.rsqrt(lax.optimization_barrier(jnp.mean(values * values, axis=-1, keepdims=True)) + EPS) * scale_vec

def reference(tokens, counts, selected, router_w, pre_gain, post_gain, gate_w, up_w, down_w):
    shard_count = counts.shape[0]
    tok_rows = tokens.shape[0] // shard_count
    total_rows = shard_count * LOAD
    ends = jnp.cumsum(counts).astype(jnp.int32)
    starts = (ends - counts).astype(jnp.int32)
    global_row = jnp.arange(total_rows, dtype=jnp.int32)
    owner = lax.optimization_barrier(jnp.sum((ends[None, :] <= global_row[:, None]).astype(jnp.int32), axis=1)).astype(jnp.int32)
    within = (global_row - starts[owner]).astype(jnp.int32)
    position = (selected[owner, within] + owner * tok_rows).astype(jnp.int32)
    work_rows = tokens[position].astype(jnp.float32)
    weight = jax.nn.sigmoid(jnp.dot(work_rows, router_w, precision=lax.Precision.HIGHEST))
    normed = norm_rows(work_rows, pre_gain).astype(jnp.bfloat16)
    gate_part = jnp.dot(normed, gate_w, preferred_element_type=jnp.float32)
    up_part = jnp.dot(normed, up_w, preferred_element_type=jnp.float32)
    hidden = (jax.nn.gelu(gate_part, approximate=True) * up_part).astype(jnp.bfloat16)
    mixed = jnp.dot(hidden, down_w, preferred_element_type=jnp.float32)
    update = weight[:, None] * norm_rows(mixed, post_gain)
    result = tokens.astype(jnp.float32).at[position].add(update)
    return result.astype(jnp.bfloat16)
```

```python
import jax
import jax.numpy as jnp
from jax import lax
from jax.sharding import PartitionSpec as P

EPS = 1e-06
DEAD = 16384.0
BF16 = jnp.bfloat16
F32 = jnp.float32


def swap(value, axis, bits):
    size = lax.axis_size(axis)
    return lax.ppermute(value, axis, [(i, i ^ bits) for i in range(size)])


def body(tokens, counts, selected, router_w, pre_gain, post_gain, gate_w, up_w, down_w):
    tok_rows, width = tokens.shape
    capacity = selected.shape[1]
    shards = lax.axis_size("seq")
    pair_count = lax.axis_size("tp")
    total = shards * capacity // 2
    piece = width // pair_count
    seq_index = lax.axis_index("seq")
    tp_index = lax.axis_index("tp")

    is_live = jnp.arange(capacity) < counts[0]
    picker = ((selected[0][:, None] == jnp.arange(tok_rows)[None, :]) & is_live[:, None]).astype(BF16)
    rows_float = jnp.dot(picker, tokens, preferred_element_type=F32)
    weight = jax.nn.sigmoid(jnp.dot(rows_float, router_w, precision=lax.Precision.HIGHEST))
    scale = lax.rsqrt(jnp.mean(rows_float * rows_float, axis=-1, keepdims=True) + EPS)
    normed = jnp.where(is_live[:, None], rows_float * scale * pre_gain, DEAD).astype(BF16)
    own = lax.dynamic_slice_in_dim(normed, tp_index * piece, piece, 1)

    held = {0: own}
    for far in range(2, shards, 2):
        held[far] = swap(own, "seq", far)
    for far in range(0, shards, 2):
        held[far + 1] = swap(held[far], "seq", 1)
    pieces = jnp.concatenate([held[far] for far in range(shards)], 0)

    live = jnp.stack([held[far][:, 0] for far in range(shards)]).astype(F32) < DEAD / 2
    number = jnp.sum(live.astype(jnp.int32), axis=1)
    order = seq_index ^ jnp.arange(shards)
    first = jnp.sum(jnp.where(order[None, :] < order[:, None], number[None, :], 0), axis=1)
    slot = jnp.arange(capacity)
    target = jnp.where(slot[None, :] < number[:, None], first[:, None] + slot[None, :], -1).reshape(-1)
    pack = (jnp.arange(total)[:, None] == target[None, :]).astype(BF16)
    packed = jnp.dot(pack, pieces, preferred_element_type=F32).astype(BF16)

    parts = {0: packed}
    bits = 1
    segment = jnp.zeros((total, width), BF16)
    near = {0: packed, 1: swap(packed, "tp", 1)}
    near[2] = swap(packed, "tp", 2)
    near[3] = swap(near[2], "tp", 1)
    for k in range(pair_count):
        segment = lax.dynamic_update_slice_in_dim(segment, near[k], (tp_index ^ k) * piece, 1)

    gate_part = jnp.dot(segment, gate_w, preferred_element_type=F32)
    up_part = jnp.dot(segment, up_w, preferred_element_type=F32)
    hidden = (jax.nn.gelu(gate_part, approximate=True) * up_part).astype(BF16)
    mixed = jnp.dot(hidden, down_w, preferred_element_type=F32)

    def quarter(k):
        return lax.dynamic_slice_in_dim(mixed, (tp_index ^ k) * piece, piece, 1)

    away = swap(jnp.stack([quarter(1), quarter(3)]).astype(BF16), "tp", 1)
    far_sum = (quarter(2) + away[1].astype(F32)).astype(BF16)
    near_sum = quarter(0) + away[0].astype(F32)
    quarter_sum = (near_sum + swap(far_sum, "tp", 2).astype(F32)).astype(BF16)
    windows = jnp.dot(pack.T, quarter_sum, preferred_element_type=F32).astype(BF16)
    windows = windows.reshape(shards, capacity, piece)
    final = None
    for far in range(0, shards, 2):
        pair_sum = windows[far].astype(F32) + swap(windows[far + 1], "seq", 1).astype(F32)
        if far:
            pair_sum = swap(pair_sum.astype(BF16), "seq", far).astype(F32)
        final = pair_sum if final is None else final + pair_sum
    update = lax.all_gather(final.astype(BF16), "tp", axis=1, tiled=True).astype(F32)
    update = weight[:, None] * update * lax.rsqrt(jnp.mean(update * update, axis=-1, keepdims=True) + EPS) * post_gain
    scattered = jnp.dot(picker.T, update.astype(BF16), preferred_element_type=F32)
    return (tokens.astype(F32) + scattered).astype(BF16)


def solution(mesh):
    in_specs = (
        P("seq", None),
        P("seq"),
        P("seq", None),
        P(),
        P(),
        P(),
        P(None, ("seq", "tp")),
        P(None, ("seq", "tp")),
        P(("seq", "tp"), None),
    )
    return jax.shard_map(body, mesh=mesh, in_specs=in_specs, out_specs=P("seq", None), check_vma=False)
```

```python
from functools import partial

import jax
import jax.numpy as jnp
from jax import lax
from jax.experimental import pallas as pl
from jax.experimental.pallas import tpu as pltpu
from jax.sharding import PartitionSpec as P

EPS = 1e-06
DEAD = 16384.0
LANES = 128
BF16 = jnp.bfloat16
F32 = jnp.float32
VMEM = pl.BlockSpec(memory_space=pltpu.VMEM)
SMEM = pl.BlockSpec(memory_space=pltpu.SMEM)
HBM = pl.BlockSpec(memory_space=pltpu.HBM)
CHUNKS = 4


def swap(value, axis, bits):
    size = lax.axis_size(axis)
    return lax.ppermute(value, axis, [(i, i ^ bits) for i in range(size)])


def iota(shape, dim):
    return lax.broadcasted_iota(jnp.int32, shape, dim)


def dot_f32(left, right):
    return jnp.dot(left, right, preferred_element_type=F32)


def dot_rows(left, right):
    return lax.dot_general(left, right, (((0,), (0,)), ((), ())), preferred_element_type=F32)


def picker(chosen, count, tok_rows):
    shape = (tok_rows, chosen.shape[1])
    hit = (iota(shape, 0) == chosen) & (iota(shape, 1) < count)
    return jnp.where(hit, 1.0, 0.0).astype(BF16)


def chunks(width):
    step = width // CHUNKS
    return [(part, slice(part * step, (part + 1) * step)) for part in range(CHUNKS)]


def scaled(values, gain):
    parts = [values[:, i * LANES : (i + 1) * LANES] * gain[i : i + 1, :] for i in range(gain.shape[0])]
    return jnp.concatenate(parts, 1)


def prepare_kernel(counts, tp_at, seq_at, chosen, tokens, gain, own, rows, chosen_v, tokens_v, gain_v, done, sems):
    del seq_at
    capacity, piece = own.shape
    width = tokens.shape[1]
    copies = [
        pltpu.make_async_copy(tokens.at[:, at], tokens_v.at[:, at], sems.at[part]) for part, at in chunks(width)
    ]
    small = [
        pltpu.make_async_copy(chosen, chosen_v, done.at[0]),
        pltpu.make_async_copy(gain, gain_v, done.at[1]),
    ]
    for copy in small[:1] + copies + small[1:]:
        copy.start()
    small[0].wait()
    picked = picker(chosen_v[...], counts[0], tokens.shape[0])
    square = jnp.zeros((capacity, 1), F32)
    for part, at in chunks(width):
        copies[part].wait()
        values = dot_rows(picked, tokens_v[:, at])
        rows[:, at] = values.astype(BF16)
        square = square + jnp.sum(values * values, axis=1, keepdims=True)
    small[1].wait()
    scale = lax.rsqrt(square / width + EPS)
    live = iota((capacity, 1), 0) < counts[0]
    for i in range(piece // LANES):
        at = pl.multiple_of(tp_at[0] * piece + i * LANES, LANES)
        part = rows[:, pl.ds(at, LANES)].astype(F32) * scale
        part = part * gain_v[pl.ds(tp_at[0] * (piece // LANES) + i, 1), :]
        own[:, i * LANES : (i + 1) * LANES] = jnp.where(live, part, DEAD).astype(BF16)


def weight_kernel(rows, router_w, weight):
    logit = jnp.sum(scaled(rows[...].astype(F32), router_w[...]), axis=1, keepdims=True)
    weight[...] = jnp.broadcast_to(jax.nn.sigmoid(logit), weight.shape)


def pack_kernel(seq_at, *refs):
    pieces, (packed, places) = refs[:-2], refs[-2:]
    capacity = pieces[0].shape[0]
    held = jnp.concatenate([ref[...] for ref in pieces], 0)
    count = held.shape[0]
    live = held[:, :LANES].astype(F32) < DEAD / 2
    live_bf16 = jnp.where(live, 1.0, 0.0).astype(BF16)
    before = (seq_at[0] ^ (iota((count, count), 1) // capacity)) < (seq_at[0] ^ (iota((count, count), 0) // capacity))
    first = dot_f32(jnp.where(before, 1.0, 0.0).astype(BF16), live_bf16).astype(jnp.int32)
    target = first + (iota((count, LANES), 0) % capacity)
    for part in range(places.shape[1] // LANES):
        hit = (target == iota((count, LANES), 1) + part * LANES) & live
        places[:, part * LANES : (part + 1) * LANES] = jnp.where(hit, 1.0, 0.0).astype(BF16)
    packed[...] = dot_rows(places[...], held).astype(BF16)


def start_kernel(tp_at, first, second, gate_w, up_w, gate_out, up_out):
    deep = first.shape[1]
    for weights, result in ((gate_w, gate_out), (up_w, up_out)):
        total = None
        for far, rows in ((0, first), (1, second)):
            at = pl.multiple_of((tp_at[0] ^ far) * deep, LANES)
            part = dot_f32(rows[...], weights[pl.ds(at, deep), :])
            total = part if total is None else total + part
        result[...] = total


def finish_kernel(tp_at, third, fourth, gate_in, up_in, gate_w, up_w, hidden):
    deep = third.shape[1]
    sums = []
    for weights, before in ((gate_w, gate_in), (up_w, up_in)):
        total = before[...]
        for far, rows in ((2, third), (3, fourth)):
            at = pl.multiple_of((tp_at[0] ^ far) * deep, LANES)
            total = total + dot_f32(rows[...], weights[pl.ds(at, deep), :])
        sums.append(total)
    hidden[...] = (jax.nn.gelu(sums[0], approximate=True) * sums[1]).astype(BF16)


def down_kernel(far, tp_at, hidden, down_w, *refs):
    result = refs[-1]
    wide = result.shape[1]
    at = pl.multiple_of((tp_at[0] ^ far) * wide, LANES)
    total = dot_f32(hidden[...], down_w[:, pl.ds(at, wide)])
    for ref in refs[:-1]:
        total = total + ref[...].astype(F32)
    result[...] = total.astype(result.dtype)


def window_kernel(near, far, places, *windows):
    total = (near[...] + far[...].astype(F32)).astype(BF16)
    capacity = windows[0].shape[0]
    for slot, window in enumerate(windows):
        rows = places[slot * capacity : (slot + 1) * capacity, :]
        window[...] = dot_f32(rows, total).astype(BF16)


def sum_kernel(*refs):
    total = refs[0][...].astype(F32)
    for ref in refs[1:-1]:
        total = total + ref[...].astype(F32)
    refs[-1][...] = total.astype(BF16)


def finish_rows_kernel(counts, tp_at, chosen, tokens, weight, gain, *refs):
    parts, (out, joined, staged, sems) = refs[:-4], refs[-4:]
    width = tokens.shape[1]
    piece = width // len(parts)
    for far, part in enumerate(parts):
        joined[:, pl.ds(pl.multiple_of((tp_at[0] ^ far) * piece, LANES), piece)] = part[...].astype(F32)
    values = joined[...]
    scale = lax.rsqrt(jnp.mean(values * values, axis=1, keepdims=True) + EPS) * weight[:, :1]
    picked = picker(chosen[...], counts[0], tokens.shape[0])
    rows = gain.shape[0] // CHUNKS
    copies = []
    for part, at in chunks(width):
        update = scaled(values[:, at] * scale, gain[part * rows : (part + 1) * rows, :]).astype(BF16)
        staged[:, at] = (tokens[:, at].astype(F32) + dot_f32(picked, update)).astype(BF16)
        copies.append(pltpu.make_async_copy(staged.at[:, at], out.at[:, at], sems.at[part]))
        copies[-1].start()
    for copy in copies:
        copy.wait()


def call(kernel, shapes, scalars, operands, flops=0, scratch=(), spec=None, out_spec=None):
    return pl.pallas_call(
        kernel,
        out_shape=shapes,
        in_specs=[SMEM] * len(scalars) + [spec or VMEM] * len(operands),
        out_specs=jax.tree.map(lambda _: out_spec or VMEM, shapes),
        scratch_shapes=scratch,
        compiler_params=pltpu.CompilerParams(vmem_limit_bytes=8 << 20),
        cost_estimate=pl.CostEstimate(flops=flops, bytes_accessed=0, transcendentals=0),
    )(*scalars, *operands)


def array(rows, columns, kind=BF16):
    return jax.ShapeDtypeStruct((rows, columns), kind)


def layer(tokens, counts, selected, router_w, pre_gain, post_gain, gate_w, up_w, down_w):
    tok_rows, width = tokens.shape
    capacity = selected.shape[1]
    shards = lax.axis_size("seq")
    pair_count = lax.axis_size("tp")
    units = gate_w.shape[1]
    total = shards * capacity // 2
    piece = width // pair_count
    seq_at = lax.axis_index("seq").astype(jnp.int32).reshape(1)
    tp_at = lax.axis_index("tp").astype(jnp.int32).reshape(1)

    own, rows = call(
        prepare_kernel,
        (array(capacity, piece), array(capacity, width)),
        (counts, tp_at, seq_at),
        [
            pltpu.with_memory_space_constraint(value, pltpu.HBM)
            for value in (selected, tokens, pre_gain.reshape(-1, LANES))
        ],
        scratch=(
            pltpu.VMEM(selected.shape, jnp.int32),
            pltpu.VMEM(tokens.shape, BF16),
            pltpu.VMEM((width // LANES, LANES), F32),
            pltpu.SemaphoreType.DMA((2,)),
            pltpu.SemaphoreType.DMA((CHUNKS,)),
        ),
        spec=HBM,
    )
    weight = call(
        weight_kernel,
        array(capacity, LANES, F32),
        (),
        (rows, router_w.reshape(-1, LANES)),
        flops=64 * total * width * units,
    )

    held = {0: own}
    for far in range(2, shards, 2):
        held[far] = swap(own, "seq", far)
    beside, weight = lax.optimization_barrier((own, weight))
    for far in range(0, shards, 2):
        held[far + 1] = swap(held[far] if far else beside, "seq", 1)
    packed, places = call(
        pack_kernel,
        (array(total, piece), array(shards * capacity, total)),
        (seq_at,),
        [held[far] for far in range(shards)],
        flops=16 * total * piece * units,
    )

    flops = 2 * total * piece * units
    third = swap(packed, "tp", 2)
    second = swap(packed, "tp", 1)
    sums = call(
        start_kernel,
        (array(total, units, F32), array(total, units, F32)),
        (tp_at,),
        (packed, second, gate_w, up_w),
        4 * flops,
    )
    third, sums = lax.optimization_barrier((third, sums))
    fourth = swap(third, "tp", 1)
    hidden = call(
        finish_kernel, array(total, units), (tp_at,), (third, fourth, *sums, gate_w, up_w), 4 * flops
    )

    def down(far, kind, *extra):
        return call(partial(down_kernel, far), array(total, piece, kind), (tp_at,), (hidden, down_w, *extra), flops)

    far_away = swap(down(3, BF16), "tp", 1)
    near_away = swap(down(1, BF16), "tp", 1)
    far_sum = swap(down(2, BF16, far_away), "tp", 2)
    near_sum = down(0, F32, near_away)
    windows = call(
        window_kernel, [array(capacity, piece)] * shards, (), (near_sum, far_sum, places)
    )
    arrived = []
    for far in range(shards - 2, 0, -2):
        other = swap(windows[far + 1], "seq", 1)
        arrived.append(swap(call(sum_kernel, array(capacity, piece), (), (windows[far], other)), "seq", far))
    other = swap(windows[1], "seq", 1)
    final = call(sum_kernel, array(capacity, piece), (), (windows[0], other, *arrived))
    other_far = swap(final, "tp", 2)
    other_near = swap(final, "tp", 1)
    last = swap(other_far, "tp", 1)
    return call(
        finish_rows_kernel,
        array(tok_rows, width),
        (counts, tp_at),
        (selected, tokens, weight, post_gain.reshape(-1, LANES), final, other_near, other_far, last),
        scratch=(
            pltpu.VMEM((capacity, width), F32),
            pltpu.VMEM(tokens.shape, BF16),
            pltpu.SemaphoreType.DMA((CHUNKS,)),
        ),
        out_spec=HBM,
    )


def solution(mesh):
    in_specs = (
        P("seq", None),
        P("seq"),
        P("seq", None),
        P(),
        P(),
        P(),
        P(None, ("seq", "tp")),
        P(None, ("seq", "tp")),
        P(("seq", "tp"), None),
    )
    return jax.shard_map(layer, mesh=mesh, in_specs=in_specs, out_specs=P("seq", None), check_vma=False)
```

```python
from functools import partial

import jax
import jax.numpy as jnp
from jax import lax
from jax.experimental import pallas as pl
from jax.experimental.pallas import tpu as pltpu
from jax.sharding import PartitionSpec as P

EPS = 1e-06
DEAD = 16384.0
LANES = 128
BF16 = jnp.bfloat16
F32 = jnp.float32
VMEM = pl.BlockSpec(memory_space=pltpu.VMEM)
SMEM = pl.BlockSpec(memory_space=pltpu.SMEM)
HBM = pl.BlockSpec(memory_space=pltpu.HBM)
CHUNKS = 4
TP = 4


def swap(value, axis, bits):
    size = lax.axis_size(axis)
    return lax.ppermute(value, axis, [(i, i ^ bits) for i in range(size)])


def iota(shape, dim):
    return lax.broadcasted_iota(jnp.int32, shape, dim)


def dot_f32(left, right):
    return jnp.dot(left, right, preferred_element_type=F32)


def dot_rows(left, right):
    return lax.dot_general(left, right, (((0,), (0,)), ((), ())), preferred_element_type=F32)


def picker(chosen, count, tok_rows):
    shape = (tok_rows, chosen.shape[1])
    hit = (iota(shape, 0) == chosen) & (iota(shape, 1) < count)
    return jnp.where(hit, 1.0, 0.0).astype(BF16)


def chunks(width):
    step = width // CHUNKS
    return [(part, slice(part * step, (part + 1) * step)) for part in range(CHUNKS)]


def scaled(values, gain):
    parts = [values[:, i * LANES : (i + 1) * LANES] * gain[i : i + 1, :] for i in range(gain.shape[0])]
    return jnp.concatenate(parts, 1)


def prepare_kernel(
    counts, tp_at, seq_at, chosen, tokens, gain, router_w,
    own, rows, picked, router_v, chosen_v, tokens_v, gain_v, done, sems,
):
    del seq_at
    capacity, piece = own.shape
    width = tokens.shape[1]
    copies = [
        pltpu.make_async_copy(tokens.at[:, at], tokens_v.at[:, at], sems.at[part]) for part, at in chunks(width)
    ]
    small = [
        pltpu.make_async_copy(source, target, done.at[at])
        for at, (source, target) in enumerate(
            ((chosen, chosen_v), (gain, gain_v), (router_w, router_v))
        )
    ]
    for copy in small[:1] + copies + small[1:]:
        copy.start()
    small[0].wait()
    count = counts[0]
    picked[...] = picker(chosen_v[...], count, tokens.shape[0])
    hot = picked[...]
    square = jnp.zeros((capacity, 1), F32)
    for part, at in chunks(width):
        copies[part].wait()
        values = dot_rows(hot, tokens_v[:, at])
        rows[:, at] = values.astype(BF16)
        square = square + jnp.sum(values * values, axis=1, keepdims=True)
    small[1].wait()
    scale = lax.rsqrt(square / width + EPS)
    live = iota((capacity, 1), 0) < count
    for i in range(piece // LANES):
        at = pl.multiple_of(tp_at[0] * piece + i * LANES, LANES)
        part = rows[:, pl.ds(at, LANES)].astype(F32) * scale
        part = part * gain_v[pl.ds(tp_at[0] * (piece // LANES) + i, 1), :]
        own[:, i * LANES : (i + 1) * LANES] = jnp.where(live, part, DEAD).astype(BF16)
    small[2].wait()


def weight_kernel(rows, router_w, weight):
    logit = jnp.sum(scaled(rows[...].astype(F32), router_w[...]), axis=1, keepdims=True)
    weight[...] = jnp.broadcast_to(jax.nn.sigmoid(logit), weight.shape)


def pack_kernel(seq_at, *refs):
    pieces, (packed, places, *halves) = refs[:-4], refs[-4:]
    capacity = pieces[0].shape[0]
    held = jnp.concatenate([ref[...] for ref in pieces], 0)
    count = held.shape[0]
    live = held[:, :LANES].astype(F32) < DEAD / 2
    live_bf16 = jnp.where(live, 1.0, 0.0).astype(BF16)
    block = min(count, 2 * LANES)
    firsts = []
    for top in range(0, count, block):
        shard = seq_at[0] ^ ((iota((block, count), 0) + top) // capacity)
        before = (seq_at[0] ^ (iota((block, count), 1) // capacity)) < shard
        firsts.append(dot_f32(jnp.where(before, 1.0, 0.0).astype(BF16), live_bf16).astype(jnp.int32))
    first = jnp.concatenate(firsts, 0)
    target = first + (iota((count, LANES), 0) % capacity)
    for part in range(places.shape[1] // LANES):
        hit = (target == iota((count, LANES), 1) + part * LANES) & live
        places[:, part * LANES : (part + 1) * LANES] = jnp.where(hit, 1.0, 0.0).astype(BF16)
    packed[...] = dot_rows(places[...], held).astype(BF16)
    cut = halves[0].shape[1]
    halves[0][...] = packed[:, :cut]
    halves[1][...] = packed[:, cut:]


def gated(tp_at, far, rows, weights, at=0):
    deep = weights.shape[0] // TP
    start = pl.multiple_of((tp_at[0] ^ far) * deep + at, LANES)
    return dot_f32(rows[...], weights[pl.ds(start, rows.shape[1]), :])


def start_kernel(tp_at, first, second, gate_w, up_w, down_w, gate_out, up_out):
    del down_w
    for weights, result in ((gate_w, gate_out), (up_w, up_out)):
        result[...] = gated(tp_at, 0, first, weights) + gated(tp_at, 1, second, weights)


def middle_kernel(places, tp_at, *refs):
    rows, (gate_in, up_in, gate_w, up_w, gate_out, up_out) = refs[:-6], refs[-6:]
    for weights, before, result in ((gate_w, gate_in, gate_out), (up_w, up_in, up_out)):
        total = before[...]
        for (far, at), part in zip(places, rows):
            total = total + gated(tp_at, far, part, weights, at)
        result[...] = total


def finish_kernel(place, tp_at, rows, gate_in, up_in, gate_w, up_w, hidden):
    far, at = place
    gate = gate_in[...] + gated(tp_at, far, rows, gate_w, at)
    up = up_in[...] + gated(tp_at, far, rows, up_w, at)
    hidden[...] = (jax.nn.gelu(gate, approximate=True) * up).astype(BF16)


def down_kernel(far, offset, tp_at, hidden, down_w, *refs):
    result = refs[-1]
    wide = result.shape[1]
    at = pl.multiple_of((tp_at[0] ^ far) * (down_w.shape[1] // TP) + offset, LANES)
    total = dot_f32(hidden[...], down_w[:, pl.ds(at, wide)])
    for ref in refs[:-1]:
        total = total + ref[...].astype(F32)
    result[...] = total.astype(result.dtype)


def window_kernel(near, first, second, places, *windows):
    total = near[...] + jnp.concatenate([first[...], second[...]], 1).astype(F32)
    total = total.astype(BF16)
    first = 0
    for window in windows:
        count = window.shape[0]
        window[...] = dot_f32(places[first : first + count, :], total).astype(BF16)
        first += count


def add_up(values, refs):
    total = values.astype(F32)
    for ref in refs:
        total = total + ref[...].astype(F32)
    return total.astype(BF16)


def sum_kernel(first, *refs):
    refs[-1][...] = add_up(first[...], refs[:-1])


def late_kernel(pair, *refs):
    refs[-1][...] = add_up(pair[refs[-1].shape[0] :, :], refs[:-1])


def last_kernel(pair, *refs):
    refs[-1][...] = add_up(pair[: refs[-1].shape[0], :], refs[:-1])


def finish_rows_kernel(tp_at, picked, tokens, weight, gain, *refs):
    parts, (out, joined, staged, sems) = refs[:-4], refs[-4:]
    width = tokens.shape[1]
    piece = width // len(parts)
    for far, part in enumerate(parts):
        joined[:, pl.ds(pl.multiple_of((tp_at[0] ^ far) * piece, LANES), piece)] = part[...].astype(F32)
    values = joined[...]
    scale = lax.rsqrt(jnp.mean(values * values, axis=1, keepdims=True) + EPS) * weight[:, :1]
    hot = picked[...]
    rows = gain.shape[0] // CHUNKS
    copies = []
    for part, at in chunks(width):
        update = scaled(values[:, at] * scale, gain[part * rows : (part + 1) * rows, :]).astype(BF16)
        staged[:, at] = (tokens[:, at].astype(F32) + dot_f32(hot, update)).astype(BF16)
        copies.append(pltpu.make_async_copy(staged.at[:, at], out.at[:, at], sems.at[part]))
        copies[-1].start()
    for copy in copies:
        copy.wait()


def call(kernel, shapes, scalars, operands, flops=0, scratch=(), spec=None, out_spec=None):
    return pl.pallas_call(
        kernel,
        out_shape=shapes,
        in_specs=[SMEM] * len(scalars) + [spec or VMEM] * len(operands),
        out_specs=jax.tree.map(lambda _: out_spec or VMEM, shapes),
        scratch_shapes=scratch,
        compiler_params=pltpu.CompilerParams(vmem_limit_bytes=min(32, lax.axis_size("seq")) << 20),
        cost_estimate=pl.CostEstimate(flops=flops, bytes_accessed=0, transcendentals=0),
    )(*scalars, *operands)


def array(rows, columns, kind=BF16):
    return jax.ShapeDtypeStruct((rows, columns), kind)


def layer(tokens, counts, selected, router_w, pre_gain, post_gain, gate_w, up_w, down_w):
    tok_rows, width = tokens.shape
    capacity = selected.shape[1]
    shards = lax.axis_size("seq")
    pair_count = lax.axis_size("tp")
    units = gate_w.shape[1]
    total = shards * capacity // 2
    piece = width // pair_count
    seq_at = lax.axis_index("seq").astype(jnp.int32).reshape(1)
    tp_at = lax.axis_index("tp").astype(jnp.int32).reshape(1)

    own, rows, picked, router_v = call(
        prepare_kernel,
        (
            array(capacity, piece),
            array(capacity, width),
            array(tok_rows, capacity),
            array(width // LANES, LANES, F32),
        ),
        (counts, tp_at, seq_at),
        [
            pltpu.with_memory_space_constraint(value, pltpu.HBM)
            for value in (
                selected, tokens, pre_gain.reshape(-1, LANES), router_w.reshape(-1, LANES)
            )
        ],
        scratch=(
            pltpu.VMEM(selected.shape, jnp.int32),
            pltpu.VMEM(tokens.shape, BF16),
            pltpu.VMEM((width // LANES, LANES), F32),
            pltpu.SemaphoreType.DMA((3,)),
            pltpu.SemaphoreType.DMA((CHUNKS,)),
        ),
        spec=HBM,
    )
    weight = call(
        weight_kernel,
        array(capacity, LANES, F32),
        (),
        (rows, router_v),
        flops=64 * total * width * units,
    )

    held = {0: own}
    for far in range(2, shards, 2):
        held[far] = swap(own, "seq", far)
    held[1] = swap(own, "seq", 1)
    held[shards - 2], weight = lax.optimization_barrier((held[shards - 2], weight))
    held[3] = swap(held[1], "seq", 2)
    for far in range(4, shards, 2):
        held[far + 1] = swap(held[far], "seq", 1)
    assert pair_count == TP
    cut = (piece // LANES + 1) // 2 * LANES
    cuts = (0, cut), (cut, piece - cut)
    packed, places, *halves = call(
        pack_kernel,
        (array(total, piece), array(shards * capacity, total), *[array(total, wide) for _, wide in cuts]),
        (seq_at,),
        [held[far] for far in range(shards)],
        flops=16 * total * piece * units,
    )

    flops = 2 * total * piece * units
    part = (array(total, units, F32), array(total, units, F32))
    third = [swap(rows, "tp", 2) for rows in halves]
    second = swap(packed, "tp", 1)
    sums = call(start_kernel, part, (tp_at,), (packed, second, gate_w, up_w, down_w), 4 * flops)
    third[0], sums = lax.optimization_barrier((third[0], sums))
    fourth = [swap(third[0], "tp", 1)]
    sums = call(partial(middle_kernel, ((2, 0),)), part, (tp_at,), (third[0], *sums, gate_w, up_w), flops)
    third[1], sums = lax.optimization_barrier((third[1], sums))
    fourth.append(swap(third[1], "tp", 1))
    sums = call(
        partial(middle_kernel, ((3, 0), (2, cut))), part, (tp_at,), (fourth[0], third[1], *sums, gate_w, up_w), flops
    )
    fourth[1], sums = lax.optimization_barrier((fourth[1], sums))
    hidden = call(
        partial(finish_kernel, (3, cut)), array(total, units), (tp_at,), (fourth[1], *sums, gate_w, up_w), flops
    )

    def down(far, kind, at, wide, *extra):
        kernel = partial(down_kernel, far, at)
        return call(kernel, array(total, wide, kind), (tp_at,), (hidden, down_w, *extra), flops // 2)

    far_sums = []
    for at, wide in cuts:
        away = swap(down(3, BF16, at, wide), "tp", 1)
        mine = down(2, F32, at, wide)
        away, mine = lax.optimization_barrier((away, mine))
        far_sum = call(sum_kernel, array(total, wide), (), (mine, away))
        far_sums.append(swap(far_sum, "tp", 2))
    near_away = swap(down(1, BF16, 0, piece), "tp", 1)
    near_sum = down(0, F32, 0, piece, near_away)
    one = array(capacity, piece)
    shapes = [one, one, array(2 * capacity, piece)] + [one] * (shards - 4)
    windows = call(window_kernel, shapes, (), (near_sum, *far_sums, places))
    ready = []
    for far in range(shards - 2, 2, -2):
        other = swap(windows[far], "seq", 1)
        pair = call(sum_kernel, one, (), (windows[far - 1], other))
        ready.append(swap(pair, "seq", far))
    pair = swap(windows[2], "seq", 2)
    other = swap(call(late_kernel, one, (), (pair, windows[1])), "seq", 1)
    final = call(last_kernel, one, (), (pair, windows[0], other, *ready))
    other_far = swap(final, "tp", 2)
    other_near = swap(final, "tp", 1)
    last = swap(other_far, "tp", 1)
    return call(
        finish_rows_kernel,
        array(tok_rows, width),
        (tp_at,),
        (picked, tokens, weight, post_gain.reshape(-1, LANES), final, other_near, other_far, last),
        scratch=(
            pltpu.VMEM((capacity, width), F32),
            pltpu.VMEM(tokens.shape, BF16),
            pltpu.SemaphoreType.DMA((CHUNKS,)),
        ),
        out_spec=HBM,
    )


def solution(mesh):
    in_specs = (
        P("seq", None),
        P("seq"),
        P("seq", None),
        P(),
        P(),
        P(),
        P(None, ("seq", "tp")),
        P(None, ("seq", "tp")),
        P(("seq", "tp"), None),
    )
    return jax.shard_map(layer, mesh=mesh, in_specs=in_specs, out_specs=P("seq", None), check_vma=False)
```

```python
from functools import partial

import jax
import jax.numpy as jnp
from jax import lax
from jax.experimental import pallas as pl
from jax.experimental.pallas import tpu as pltpu
from jax.sharding import PartitionSpec as P

EPS = 1e-06
DEAD = 16384.0
LANES = 128
BF16 = jnp.bfloat16
F32 = jnp.float32
VMEM = pl.BlockSpec(memory_space=pltpu.VMEM)
SMEM = pl.BlockSpec(memory_space=pltpu.SMEM)
HBM = pl.BlockSpec(memory_space=pltpu.HBM)
CHUNKS = 1
OUT_CHUNKS = 4
TP = 4


def swap(value, axis, bits):
    size = lax.axis_size(axis)
    return lax.ppermute(value, axis, [(i, i ^ bits) for i in range(size)])


def iota(shape, dim):
    return lax.broadcasted_iota(jnp.int32, shape, dim)


def dot_f32(left, right):
    return jnp.dot(left, right, preferred_element_type=F32)


def dot_rows(left, right):
    return lax.dot_general(left, right, (((0,), (0,)), ((), ())), preferred_element_type=F32)


def picker(chosen, count, tok_rows):
    shape = (tok_rows, chosen.shape[1])
    hit = (iota(shape, 0) == chosen) & (iota(shape, 1) < count)
    return jnp.where(hit, 1.0, 0.0).astype(BF16)


def chunks(width, count):
    step = width // count
    return [(part, slice(part * step, (part + 1) * step)) for part in range(count)]


def scaled(values, gain):
    parts = [values[:, i * LANES : (i + 1) * LANES] * gain[i : i + 1, :] for i in range(gain.shape[0])]
    return jnp.concatenate(parts, 1)


def prepare_kernel(
    counts, tp_at, seq_at, chosen, tokens, gain, router_w,
    own, rows, picked, router_v, chosen_v, tokens_v, gain_v, done, sems,
):
    del seq_at
    capacity, piece = own.shape
    width = tokens.shape[1]
    copies = [
        pltpu.make_async_copy(tokens.at[:, at], tokens_v.at[:, at], sems.at[part]) for part, at in chunks(width, CHUNKS)
    ]
    small = [
        pltpu.make_async_copy(source, target, done.at[at])
        for at, (source, target) in enumerate(
            ((chosen, chosen_v), (gain, gain_v), (router_w, router_v))
        )
    ]
    for copy in small[:1] + copies + small[1:]:
        copy.start()
    small[0].wait()
    count = counts[0]
    picked[...] = picker(chosen_v[...], count, tokens.shape[0])
    hot = picked[...].astype(F32).T.astype(BF16)
    square = jnp.zeros((capacity, 1), F32)
    for part, at in chunks(width, CHUNKS):
        copies[part].wait()
        values = dot_f32(hot, tokens_v[:, at])
        rows[:, at] = values.astype(BF16)
        square = square + jnp.sum(values * values, axis=1, keepdims=True)
    small[1].wait()
    scale = lax.rsqrt(square / width + EPS)
    live = iota((capacity, 1), 0) < count
    for i in range(piece // LANES):
        at = pl.multiple_of(tp_at[0] * piece + i * LANES, LANES)
        part = rows[:, pl.ds(at, LANES)].astype(F32) * scale
        part = part * gain_v[pl.ds(tp_at[0] * (piece // LANES) + i, 1), :]
        own[:, i * LANES : (i + 1) * LANES] = jnp.where(live, part, DEAD).astype(BF16)
    small[2].wait()


def weight_kernel(rows, router_w, weight):
    logit = jnp.sum(scaled(rows[...].astype(F32), router_w[...]), axis=1, keepdims=True)
    weight[...] = jnp.broadcast_to(jax.nn.sigmoid(logit), weight.shape)


def pack_kernel(seq_at, *refs):
    pieces, (packed, places, *halves) = refs[:-4], refs[-4:]
    capacity = pieces[0].shape[0]
    held = jnp.concatenate([ref[...] for ref in pieces], 0)
    count = held.shape[0]
    live = held[:, :LANES].astype(F32) < DEAD / 2
    live_bf16 = jnp.where(live, 1.0, 0.0).astype(BF16)
    block = min(count, 2 * LANES)
    firsts = []
    for top in range(0, count, block):
        shard = seq_at[0] ^ ((iota((block, count), 0) + top) // capacity)
        before = (seq_at[0] ^ (iota((block, count), 1) // capacity)) < shard
        firsts.append(dot_f32(jnp.where(before, 1.0, 0.0).astype(BF16), live_bf16).astype(jnp.int32))
    first = jnp.concatenate(firsts, 0)
    target = first + (iota((count, LANES), 0) % capacity)
    for part in range(places.shape[1] // LANES):
        hit = (target == iota((count, LANES), 1) + part * LANES) & live
        places[:, part * LANES : (part + 1) * LANES] = jnp.where(hit, 1.0, 0.0).astype(BF16)
    packed[...] = dot_rows(places[...], held).astype(BF16)
    cut = halves[0].shape[1]
    halves[0][...] = packed[:, :cut]
    halves[1][...] = packed[:, cut:]


def gated(tp_at, far, rows, weights, at=0):
    deep = weights.shape[0] // TP
    start = pl.multiple_of((tp_at[0] ^ far) * deep + at, LANES)
    return dot_f32(rows[...], weights[pl.ds(start, rows.shape[1]), :])


def start_kernel(tp_at, first, second, gate_w, up_w, down_w, gate_out, up_out):
    del down_w
    for weights, result in ((gate_w, gate_out), (up_w, up_out)):
        result[...] = gated(tp_at, 0, first, weights) + gated(tp_at, 1, second, weights)


def middle_kernel(places, tp_at, *refs):
    rows, (gate_in, up_in, gate_w, up_w, gate_out, up_out) = refs[:-6], refs[-6:]
    for weights, before, result in ((gate_w, gate_in, gate_out), (up_w, up_in, up_out)):
        total = before[...]
        for (far, at), part in zip(places, rows):
            total = total + gated(tp_at, far, part, weights, at)
        result[...] = total


def finish_kernel(place, tp_at, rows, gate_in, up_in, gate_w, up_w, hidden):
    far, at = place
    gate = gate_in[...] + gated(tp_at, far, rows, gate_w, at)
    up = up_in[...] + gated(tp_at, far, rows, up_w, at)
    hidden[...] = (jax.nn.gelu(gate, approximate=True) * up).astype(BF16)


def down_kernel(far, offset, tp_at, hidden, down_w, *refs):
    result = refs[-1]
    wide = result.shape[1]
    at = pl.multiple_of((tp_at[0] ^ far) * (down_w.shape[1] // TP) + offset, LANES)
    total = dot_f32(hidden[...], down_w[:, pl.ds(at, wide)])
    for ref in refs[:-1]:
        total = total + ref[...].astype(F32)
    result[...] = total.astype(result.dtype)


def window_kernel(near, first, second, places, *windows):
    total = near[...] + jnp.concatenate([first[...], second[...]], 1).astype(F32)
    total = total.astype(BF16)
    first = 0
    for window in windows:
        count = window.shape[0]
        window[...] = dot_f32(places[first : first + count, :], total).astype(BF16)
        first += count


def add_up(values, refs):
    total = values.astype(F32)
    for ref in refs:
        total = total + ref[...].astype(F32)
    return total.astype(BF16)


def sum_kernel(first, *refs):
    refs[-1][...] = add_up(first[...], refs[:-1])


def late_kernel(pair, *refs):
    refs[-1][...] = add_up(pair[refs[-1].shape[0] :, :], refs[:-1])


def last_kernel(pair, *refs):
    refs[-1][...] = add_up(pair[: refs[-1].shape[0], :], refs[:-1])


def finish_rows_kernel(tp_at, picked, tokens, weight, gain, *refs):
    parts, (out, joined, staged, sems) = refs[:-4], refs[-4:]
    width = tokens.shape[1]
    piece = width // len(parts)
    for far, part in enumerate(parts):
        joined[:, pl.ds(pl.multiple_of((tp_at[0] ^ far) * piece, LANES), piece)] = part[...].astype(F32)
    values = joined[...]
    scale = lax.rsqrt(jnp.mean(values * values, axis=1, keepdims=True) + EPS) * weight[:, :1]
    hot = picked[...]
    rows = gain.shape[0] // OUT_CHUNKS
    copies = []
    for part, at in chunks(width, OUT_CHUNKS):
        update = scaled(values[:, at] * scale, gain[part * rows : (part + 1) * rows, :]).astype(BF16)
        staged[:, at] = (tokens[:, at].astype(F32) + dot_f32(hot, update)).astype(BF16)
        copies.append(pltpu.make_async_copy(staged.at[:, at], out.at[:, at], sems.at[part]))
        copies[-1].start()
    for copy in copies:
        copy.wait()


def call(kernel, shapes, scalars, operands, flops=0, scratch=(), spec=None, out_spec=None):
    return pl.pallas_call(
        kernel,
        out_shape=shapes,
        in_specs=[SMEM] * len(scalars) + [spec or VMEM] * len(operands),
        out_specs=jax.tree.map(lambda _: out_spec or VMEM, shapes),
        scratch_shapes=scratch,
        compiler_params=pltpu.CompilerParams(vmem_limit_bytes=min(32, lax.axis_size("seq")) << 20),
        cost_estimate=pl.CostEstimate(flops=flops, bytes_accessed=0, transcendentals=0),
    )(*scalars, *operands)


def array(rows, columns, kind=BF16):
    return jax.ShapeDtypeStruct((rows, columns), kind)


def layer(tokens, counts, selected, router_w, pre_gain, post_gain, gate_w, up_w, down_w):
    tok_rows, width = tokens.shape
    capacity = selected.shape[1]
    shards = lax.axis_size("seq")
    pair_count = lax.axis_size("tp")
    units = gate_w.shape[1]
    total = shards * capacity // 2
    piece = width // pair_count
    seq_at = lax.axis_index("seq").astype(jnp.int32).reshape(1)
    tp_at = lax.axis_index("tp").astype(jnp.int32).reshape(1)

    own, rows, picked, router_v = call(
        prepare_kernel,
        (
            array(capacity, piece),
            array(capacity, width),
            array(tok_rows, capacity),
            array(width // LANES, LANES, F32),
        ),
        (counts, tp_at, seq_at),
        [
            pltpu.with_memory_space_constraint(value, pltpu.HBM)
            for value in (
                selected, tokens, pre_gain.reshape(-1, LANES), router_w.reshape(-1, LANES)
            )
        ],
        scratch=(
            pltpu.VMEM(selected.shape, jnp.int32),
            pltpu.VMEM(tokens.shape, BF16),
            pltpu.VMEM((width // LANES, LANES), F32),
            pltpu.SemaphoreType.DMA((3,)),
            pltpu.SemaphoreType.DMA((CHUNKS,)),
        ),
        spec=HBM,
    )
    weight = call(
        weight_kernel,
        array(capacity, LANES, F32),
        (),
        (rows, router_v),
        flops=64 * total * width * units,
    )

    held = {0: own}
    for far in range(2, shards, 2):
        held[far] = swap(own, "seq", far)
    held[1] = swap(own, "seq", 1)
    held[shards - 2], weight = lax.optimization_barrier((held[shards - 2], weight))
    held[3] = swap(held[1], "seq", 2)
    for far in range(4, shards, 2):
        held[far + 1] = swap(held[far], "seq", 1)
    assert pair_count == TP
    cut = (piece // LANES + 1) // 2 * LANES
    cuts = (0, cut), (cut, piece - cut)
    packed, places, *halves = call(
        pack_kernel,
        (array(total, piece), array(shards * capacity, total), *[array(total, wide) for _, wide in cuts]),
        (seq_at,),
        [held[far] for far in range(shards)],
        flops=16 * total * piece * units,
    )

    flops = 2 * total * piece * units
    part = (array(total, units, F32), array(total, units, F32))
    third = [swap(rows, "tp", 2) for rows in halves]
    second = swap(packed, "tp", 1)
    sums = call(start_kernel, part, (tp_at,), (packed, second, gate_w, up_w, down_w), 4 * flops)
    third[0], sums = lax.optimization_barrier((third[0], sums))
    fourth = [swap(third[0], "tp", 1)]
    sums = call(partial(middle_kernel, ((2, 0),)), part, (tp_at,), (third[0], *sums, gate_w, up_w), flops)
    third[1], sums = lax.optimization_barrier((third[1], sums))
    fourth.append(swap(third[1], "tp", 1))
    sums = call(
        partial(middle_kernel, ((3, 0), (2, cut))), part, (tp_at,), (fourth[0], third[1], *sums, gate_w, up_w), flops
    )
    fourth[1], sums = lax.optimization_barrier((fourth[1], sums))
    hidden = call(
        partial(finish_kernel, (3, cut)), array(total, units), (tp_at,), (fourth[1], *sums, gate_w, up_w), flops
    )

    def down(far, kind, at, wide, *extra):
        kernel = partial(down_kernel, far, at)
        return call(kernel, array(total, wide, kind), (tp_at,), (hidden, down_w, *extra), flops // 2)

    far_sums = []
    for at, wide in cuts:
        away = swap(down(3, BF16, at, wide), "tp", 1)
        mine = down(2, F32, at, wide)
        away, mine = lax.optimization_barrier((away, mine))
        far_sum = call(sum_kernel, array(total, wide), (), (mine, away))
        far_sums.append(swap(far_sum, "tp", 2))
    near_away = swap(down(1, BF16, 0, piece), "tp", 1)
    near_sum = down(0, F32, 0, piece, near_away)
    one = array(capacity, piece)
    shapes = [one, one, array(2 * capacity, piece)] + [one] * (shards - 4)
    windows = call(window_kernel, shapes, (), (near_sum, *far_sums, places))
    ready = []
    for far in range(shards - 2, 2, -2):
        other = swap(windows[far], "seq", 1)
        pair = call(sum_kernel, one, (), (windows[far - 1], other))
        ready.append(swap(pair, "seq", far))
    pair = swap(windows[2], "seq", 2)
    other = swap(call(late_kernel, one, (), (pair, windows[1])), "seq", 1)
    final = call(last_kernel, one, (), (pair, windows[0], other, *ready))
    other_far = swap(final, "tp", 2)
    other_near = swap(final, "tp", 1)
    last = swap(other_far, "tp", 1)
    return call(
        finish_rows_kernel,
        array(tok_rows, width),
        (tp_at,),
        (picked, tokens, weight, post_gain.reshape(-1, LANES), final, other_near, other_far, last),
        scratch=(
            pltpu.VMEM((capacity, width), F32),
            pltpu.VMEM(tokens.shape, BF16),
            pltpu.SemaphoreType.DMA((OUT_CHUNKS,)),
        ),
        out_spec=HBM,
    )


def solution(mesh):
    in_specs = (
        P("seq", None),
        P("seq"),
        P("seq", None),
        P(),
        P(),
        P(),
        P(None, ("seq", "tp")),
        P(None, ("seq", "tp")),
        P(("seq", "tp"), None),
    )
    return jax.shard_map(layer, mesh=mesh, in_specs=in_specs, out_specs=P("seq", None), check_vma=False)
```

```python
from functools import partial

import jax
import jax.numpy as jnp
from jax import lax
from jax.experimental import pallas as pl
from jax.experimental.pallas import tpu as pltpu
from jax.sharding import PartitionSpec as P

EPS = 1e-06
DEAD = 16384.0
LANES = 128
BF16 = jnp.bfloat16
F32 = jnp.float32
VMEM = pl.BlockSpec(memory_space=pltpu.VMEM)
SMEM = pl.BlockSpec(memory_space=pltpu.SMEM)
HBM = pl.BlockSpec(memory_space=pltpu.HBM)
CHUNKS = 1
TP = 4


def swap(value, axis, bits):
    size = lax.axis_size(axis)
    return lax.ppermute(value, axis, [(i, i ^ bits) for i in range(size)])


def iota(shape, dim):
    return lax.broadcasted_iota(jnp.int32, shape, dim)


def dot_f32(left, right):
    return jnp.dot(left, right, preferred_element_type=F32)


def dot_rows(left, right):
    return lax.dot_general(left, right, (((0,), (0,)), ((), ())), preferred_element_type=F32)


def picker(chosen, count, tok_rows):
    shape = (tok_rows, chosen.shape[1])
    hit = (iota(shape, 0) == chosen) & (iota(shape, 1) < count)
    return jnp.where(hit, 1.0, 0.0).astype(BF16)


def chunks(width, count):
    step = width // count
    return [(part, slice(part * step, (part + 1) * step)) for part in range(count)]


def scaled(values, gain):
    parts = [values[:, i * LANES : (i + 1) * LANES] * gain[i : i + 1, :] for i in range(gain.shape[0])]
    return jnp.concatenate(parts, 1)


def prepare_kernel(
    counts, tp_at, seq_at, chosen, tokens, gain, router_w,
    own, rows, picked, router_v, chosen_v, tokens_v, gain_v, done, sems,
):
    del seq_at
    capacity, piece = own.shape
    width = tokens.shape[1]
    copies = [
        pltpu.make_async_copy(tokens.at[:, at], tokens_v.at[:, at], sems.at[part]) for part, at in chunks(width, CHUNKS)
    ]
    small = [
        pltpu.make_async_copy(source, target, done.at[at])
        for at, (source, target) in enumerate(
            ((chosen, chosen_v), (gain, gain_v), (router_w, router_v))
        )
    ]
    for copy in small[:1] + copies + small[1:]:
        copy.start()
    small[0].wait()
    count = counts[0]
    picked[...] = picker(chosen_v[...], count, tokens.shape[0])
    hot = picked[...].astype(F32).T.astype(BF16)
    square = jnp.zeros((capacity, 1), F32)
    for part, at in chunks(width, CHUNKS):
        copies[part].wait()
        values = dot_f32(hot, tokens_v[:, at])
        rows[:, at] = values.astype(BF16)
        square = square + jnp.sum(values * values, axis=1, keepdims=True)
    small[1].wait()
    scale = lax.rsqrt(square / width + EPS)
    live = iota((capacity, 1), 0) < count
    for i in range(piece // LANES):
        at = pl.multiple_of(tp_at[0] * piece + i * LANES, LANES)
        part = rows[:, pl.ds(at, LANES)].astype(F32) * scale
        part = part * gain_v[pl.ds(tp_at[0] * (piece // LANES) + i, 1), :]
        own[:, i * LANES : (i + 1) * LANES] = jnp.where(live, part, DEAD).astype(BF16)
    small[2].wait()


def weight_kernel(rows, router_w, weight):
    logit = jnp.sum(scaled(rows[...].astype(F32), router_w[...]), axis=1, keepdims=True)
    weight[...] = jnp.broadcast_to(jax.nn.sigmoid(logit), weight.shape)


def pack_kernel(seq_at, *refs):
    pieces, (packed, places, *halves) = refs[:-4], refs[-4:]
    capacity = pieces[0].shape[0]
    held = jnp.concatenate([ref[...] for ref in pieces], 0)
    count = held.shape[0]
    live = held[:, :LANES].astype(F32) < DEAD / 2
    amount = jnp.where(live, 1, 0)
    sizes = [
        jnp.sum(amount[k * capacity : (k + 1) * capacity, :], axis=0, keepdims=True) for k in range(len(pieces))
    ]
    firsts = []
    for k in range(len(pieces)):
        first = jnp.zeros((1, LANES), jnp.int32)
        for j in range(len(pieces)):
            first = first + jnp.where((seq_at[0] ^ j) < (seq_at[0] ^ k), sizes[j], 0)
        firsts.append(jnp.broadcast_to(first, (capacity, LANES)))
    first = jnp.concatenate(firsts, 0)
    target = first + (iota((count, LANES), 0) % capacity)
    for part in range(places.shape[1] // LANES):
        hit = (target == iota((count, LANES), 1) + part * LANES) & live
        places[:, part * LANES : (part + 1) * LANES] = jnp.where(hit, 1.0, 0.0).astype(BF16)
    packed[...] = dot_rows(places[...], held).astype(BF16)
    cut = halves[0].shape[1]
    halves[0][...] = packed[:, :cut]
    halves[1][...] = packed[:, cut:]


def gated(tp_at, far, rows, weights, at=0):
    deep = weights.shape[0] // TP
    start = pl.multiple_of((tp_at[0] ^ far) * deep + at, LANES)
    return dot_f32(rows[...], weights[pl.ds(start, rows.shape[1]), :])


def start_kernel(tp_at, first, second, gate_w, up_w, down_w, gate_out, up_out):
    del down_w
    for weights, result in ((gate_w, gate_out), (up_w, up_out)):
        result[...] = gated(tp_at, 0, first, weights) + gated(tp_at, 1, second, weights)


def middle_kernel(places, tp_at, *refs):
    rows, (gate_in, up_in, gate_w, up_w, gate_out, up_out) = refs[:-6], refs[-6:]
    for weights, before, result in ((gate_w, gate_in, gate_out), (up_w, up_in, up_out)):
        total = before[...]
        for (far, at), part in zip(places, rows):
            total = total + gated(tp_at, far, part, weights, at)
        result[...] = total


def finish_kernel(place, tp_at, rows, gate_in, up_in, gate_w, up_w, hidden):
    far, at = place
    gate = gate_in[...] + gated(tp_at, far, rows, gate_w, at)
    up = up_in[...] + gated(tp_at, far, rows, up_w, at)
    hidden[...] = (jax.nn.gelu(gate, approximate=True) * up).astype(BF16)


def down_kernel(far, offset, tp_at, hidden, down_w, *refs):
    result = refs[-1]
    wide = result.shape[1]
    at = pl.multiple_of((tp_at[0] ^ far) * (down_w.shape[1] // TP) + offset, LANES)
    total = dot_f32(hidden[...], down_w[:, pl.ds(at, wide)])
    for ref in refs[:-1]:
        total = total + ref[...].astype(F32)
    result[...] = total.astype(result.dtype)


def window_kernel(near, first, second, places, *windows):
    total = near[...] + jnp.concatenate([first[...], second[...]], 1).astype(F32)
    picked = dot_f32(places[...], total.astype(BF16)).astype(BF16)
    start = 0
    for window in windows:
        window[...] = picked[start : start + window.shape[0], :]
        start += window.shape[0]


def add_up(values, refs):
    total = values.astype(F32)
    for ref in refs:
        total = total + ref[...].astype(F32)
    return total.astype(BF16)


def sum_kernel(first, *refs):
    refs[-1][...] = add_up(first[...], refs[:-1])


def late_kernel(pair, *refs):
    refs[-1][...] = add_up(pair[refs[-1].shape[0] :, :], refs[:-1])


def last_kernel(pair, *refs):
    refs[-1][...] = add_up(pair[: refs[-1].shape[0], :], refs[:-1])


def finish_rows_kernel(tp_at, picked, tokens, weight, gain, *refs):
    parts, (out, staged, sems) = refs[:-3], refs[-3:]
    wide = parts[0].shape[1]
    tiles = wide // LANES
    values = [part[...].astype(F32) for part in parts]
    square = sum(jnp.sum(value * value, axis=1, keepdims=True) for value in values)
    scale = lax.rsqrt(square / tokens.shape[1] + EPS) * weight[:, :1]
    hot = picked[...]
    copies = []
    for far, value in enumerate(values):
        place = (tp_at[0] ^ far) * tiles
        at = pl.ds(pl.multiple_of(place * LANES, LANES), wide)
        gains = jnp.concatenate([gain[pl.ds(place + i, 1), :] for i in range(tiles)], 1)
        update = (value * scale * gains).astype(BF16)
        staged[:, at] = (tokens[:, at].astype(F32) + dot_f32(hot, update)).astype(BF16)
        copies.append(pltpu.make_async_copy(staged.at[:, at], out.at[:, at], sems.at[far]))
        copies[-1].start()
    for copy in copies:
        copy.wait()


def call(kernel, shapes, scalars, operands, flops=0, scratch=(), spec=None, out_spec=None):
    return pl.pallas_call(
        kernel,
        out_shape=shapes,
        in_specs=[SMEM] * len(scalars) + [spec or VMEM] * len(operands),
        out_specs=jax.tree.map(lambda _: out_spec or VMEM, shapes),
        scratch_shapes=scratch,
        compiler_params=pltpu.CompilerParams(vmem_limit_bytes=min(32, lax.axis_size("seq")) << 20),
        cost_estimate=pl.CostEstimate(flops=flops, bytes_accessed=0, transcendentals=0),
    )(*scalars, *operands)


def array(rows, columns, kind=BF16):
    return jax.ShapeDtypeStruct((rows, columns), kind)


def layer(tokens, counts, selected, router_w, pre_gain, post_gain, gate_w, up_w, down_w):
    tok_rows, width = tokens.shape
    capacity = selected.shape[1]
    shards = lax.axis_size("seq")
    pair_count = lax.axis_size("tp")
    units = gate_w.shape[1]
    total = shards * capacity // 2
    piece = width // pair_count
    seq_at = lax.axis_index("seq").astype(jnp.int32).reshape(1)
    tp_at = lax.axis_index("tp").astype(jnp.int32).reshape(1)

    own, rows, picked, router_v = call(
        prepare_kernel,
        (
            array(capacity, piece),
            array(capacity, width),
            array(tok_rows, capacity),
            array(width // LANES, LANES, F32),
        ),
        (counts, tp_at, seq_at),
        [
            pltpu.with_memory_space_constraint(value, pltpu.HBM)
            for value in (
                selected, tokens, pre_gain.reshape(-1, LANES), router_w.reshape(-1, LANES)
            )
        ],
        scratch=(
            pltpu.VMEM(selected.shape, jnp.int32),
            pltpu.VMEM(tokens.shape, BF16),
            pltpu.VMEM((width // LANES, LANES), F32),
            pltpu.SemaphoreType.DMA((3,)),
            pltpu.SemaphoreType.DMA((CHUNKS,)),
        ),
        spec=HBM,
    )
    weight = call(
        weight_kernel,
        array(capacity, LANES, F32),
        (),
        (rows, router_v),
        flops=64 * total * width * units,
    )

    held = {0: own}
    for far in range(2, shards, 2):
        held[far] = swap(own, "seq", far)
    held[1] = swap(own, "seq", 1)
    held[shards - 2], weight = lax.optimization_barrier((held[shards - 2], weight))
    held[3] = swap(held[1], "seq", 2)
    for far in range(4, shards, 2):
        held[far + 1] = swap(held[far], "seq", 1)
    assert pair_count == TP
    cut = (piece // LANES + 1) // 2 * LANES
    cuts = (0, cut), (cut, piece - cut)
    packed, places, *halves = call(
        pack_kernel,
        (array(total, piece), array(shards * capacity, total), *[array(total, wide) for _, wide in cuts]),
        (seq_at,),
        [held[far] for far in range(shards)],
        flops=16 * total * piece * units,
    )

    flops = 2 * total * piece * units
    part = (array(total, units, F32), array(total, units, F32))
    third = [swap(rows, "tp", 2) for rows in halves]
    second = swap(packed, "tp", 1)
    sums = call(start_kernel, part, (tp_at,), (packed, second, gate_w, up_w, down_w), 4 * flops)
    third[0], sums = lax.optimization_barrier((third[0], sums))
    fourth = [swap(third[0], "tp", 1)]
    sums = call(partial(middle_kernel, ((2, 0),)), part, (tp_at,), (third[0], *sums, gate_w, up_w), flops)
    third[1], sums = lax.optimization_barrier((third[1], sums))
    fourth.append(swap(third[1], "tp", 1))
    sums = call(
        partial(middle_kernel, ((3, 0), (2, cut))), part, (tp_at,), (fourth[0], third[1], *sums, gate_w, up_w), flops
    )
    fourth[1], sums = lax.optimization_barrier((fourth[1], sums))
    hidden = call(
        partial(finish_kernel, (3, cut)), array(total, units), (tp_at,), (fourth[1], *sums, gate_w, up_w), flops
    )

    def down(far, kind, at, wide, *extra):
        kernel = partial(down_kernel, far, at)
        return call(kernel, array(total, wide, kind), (tp_at,), (hidden, down_w, *extra), flops // 2)

    far_sums = []
    for at, wide in cuts:
        away = swap(down(3, BF16, at, wide), "tp", 1)
        mine = down(2, F32, at, wide)
        away, mine = lax.optimization_barrier((away, mine))
        far_sum = call(sum_kernel, array(total, wide), (), (mine, away))
        far_sums.append(swap(far_sum, "tp", 2))
    near_away = swap(down(1, BF16, 0, piece), "tp", 1)
    near_sum = down(0, F32, 0, piece, near_away)
    one = array(capacity, piece)
    shapes = [one, one, array(2 * capacity, piece)] + [one] * (shards - 4)
    windows = call(window_kernel, shapes, (), (near_sum, *far_sums, places))
    ready = []
    for far in range(shards - 2, 2, -2):
        other = swap(windows[far], "seq", 1)
        pair = call(sum_kernel, one, (), (windows[far - 1], other))
        ready.append(swap(pair, "seq", far))
    pair = swap(windows[2], "seq", 2)
    other = swap(call(late_kernel, one, (), (pair, windows[1])), "seq", 1)
    final = call(last_kernel, one, (), (pair, windows[0], other, *ready))
    other_far = swap(final, "tp", 2)
    other_near = swap(final, "tp", 1)
    last = swap(other_far, "tp", 1)
    return call(
        finish_rows_kernel,
        array(tok_rows, width),
        (tp_at,),
        (picked, tokens, weight, post_gain.reshape(-1, LANES), final, other_near, other_far, last),
        scratch=(pltpu.VMEM(tokens.shape, BF16), pltpu.SemaphoreType.DMA((TP,))),
        out_spec=HBM,
    )


def solution(mesh):
    in_specs = (
        P("seq", None),
        P("seq"),
        P("seq", None),
        P(),
        P(),
        P(),
        P(None, ("seq", "tp")),
        P(None, ("seq", "tp")),
        P(("seq", "tp"), None),
    )
    return jax.shard_map(layer, mesh=mesh, in_specs=in_specs, out_specs=P("seq", None), check_vma=False)
```
